256 devices in a mesh: wide: 64 (over z, y, core), narrow: 4 (over x).
Axes of the slice: x: 4, y: 4, z: 8, core: 2. Of those that a mesh axis runs over, the one named last changes fastest.
Arguments:
- calib: float32 [16384, 1024], P(('narrow', 'wide')), may hold values from -30 to 30, as said below
- weights: float32 [16384, 256], P(('narrow', 'wide')), may hold values from -6 to 6
- codes: int32 [4096, 256], P(('narrow', 'wide')), may hold values from 0 to 5
Outputs:
- refit: float32 [16384, 256], P(('narrow', 'wide'))
The draws below stay inside these ranges and needn't reach their ends.
Inputs may be any that keep to these rules, and one draw needn't show every extreme that they name: `calib`: real values.
All inputs are finite; a program needn't handle non-finite values.
Results may differ from the reference program's by a relative error of at most 0.002.
Values sent between devices are 32-bit elements; how exact they have to be, the bound alone decides.
No kernel may reach another device: no remote copies, remote signals or barrier semaphores. Data moves between devices by JAX's collectives and lax.ppermute only.
A program may use at most 64 MiB of HBM per device.

```python
import math
import jax
import jax.numpy as jnp
import numpy as np
from jax import lax

D = 16384
ROWS = 1024
OUT = 256
ITERS = 3
GROUPS = 4096


def draw_calib(key, part):
    first = jax.random.fold_in(key, 11)
    second = jax.random.fold_in(key, 12)
    scales = jnp.exp(jax.random.uniform(second, (D, 1), jnp.float32, math.log(0.5), math.log(5.0)))
    values = jax.random.normal(first, (D, ROWS), jnp.float32) * scales
    return jnp.clip(values, -30.0, 30.0)


def set_ends(result, rng, least, high):
    longest = result.shape.index(max(result.shape))
    spots = []
    for shift in (0, 1):
        where = [jax.random.randint(jax.random.fold_in(rng, axis), (), 0, length) for axis, length in enumerate(result.shape)]
        where[longest] = (where[longest] + shift) % result.shape[longest]
        spots.append(tuple(where))
    return result.at[spots[0]].set(least).at[spots[1]].set(high)


def level_of(own_key, extent, pieces, low, high):
    gain = 1.0
    for dim, shards_of in pieces:
        heights = jax.random.uniform(jax.random.fold_in(jax.random.fold_in(own_key, 6), dim), (shards_of,), jnp.float32, low / len(pieces), high / len(pieces))
        gain = gain * jnp.repeat(jnp.exp(heights), extent[dim] // shards_of).reshape((-1,) + (1,) * (len(extent) - 1 - dim))
    return gain


def gaussian(key, extent, scale, reach, split=(), held_as=jnp.bfloat16):
    result = scale * jax.random.normal(key, extent, jnp.float32)
    if split:
        result = result * level_of(key, extent, split, -0.22, 0.18)
    return jnp.clip(result, -reach, reach).astype(held_as)


def setup_inputs(seed: int = 0) -> dict:
    seeds = jax.random.split(jax.random.key(seed), 4)
    calib = draw_calib(jax.random.fold_in(seeds[3], 71), 0)
    weights = gaussian(seeds[1], (D, OUT), 1.0, 6.0, ((0, 256),), jnp.float32)
    codes = set_ends(jax.random.randint(seeds[2], (GROUPS, OUT), 0, 6), jax.random.fold_in(seeds[2], 1), 0, 5).astype(jnp.int32)
    return dict(calib=calib, weights=weights, codes=codes)


ridge_term = 1.0
PAIRS = np.array([[1, 1, 0, 0], [1, 0, 1, 0], [1, 0, 0, 1], [0, 1, 1, 0], [0, 1, 0, 1], [0, 0, 1, 1]], np.float32)


def keep_mask(codes):
    groups, columns = codes.shape
    onehot = (codes[:, :, None] == jnp.arange(6, dtype=jnp.int32)).astype(jnp.float32)
    picked = jnp.einsum("goc,ck->gko", onehot, jnp.asarray(PAIRS, dtype=jnp.float32))
    return picked.reshape(groups * 4, columns)


def reference(calib, weights, codes):
    mask = keep_mask(codes)

    def apply(vector):
        projected = lax.dot_general(calib, vector, (((0,), (0,)), ((), ())), precision=lax.Precision.HIGHEST, preferred_element_type=jnp.float32)
        back = jnp.dot(calib, projected, precision=lax.Precision.HIGHEST, preferred_element_type=jnp.float32)
        return back / ROWS + ridge_term * vector

    refit = mask * weights
    residual = mask * apply(weights - refit)
    direction = residual
    norm_now = jnp.sum(residual * residual, axis=0)
    for step in range(ITERS):
        image = mask * apply(direction)
        alpha = norm_now / jnp.sum(direction * image, axis=0)
        refit = refit + alpha * direction
        residual = residual - alpha * image
        norm_next = jnp.sum(residual * residual, axis=0)
        direction = residual + (norm_next / norm_now) * direction
        norm_now = norm_next
    return refit
```

```python
import jax
import jax.numpy as jnp
import numpy as np
from jax import lax
from jax.sharding import Mesh
from jax.sharding import PartitionSpec as P

ITERS = 3
RIDGE = 1.0
AXES = ("x", "z", "y", "core")
MESH = ("z", "y", "core", "x")
SHARED = ("z", "core")
SUMMED = ("y", "x")
LANES = 128
PAIRS = np.array(
    [[1, 1, 0, 0], [1, 0, 1, 0], [1, 0, 0, 1], [0, 1, 1, 0], [0, 1, 0, 1], [0, 0, 1, 1]], np.float32
)


def keep_mask(codes):
    groups, columns = codes.shape
    onehot = (codes[:, :, None] == jnp.arange(6, dtype=jnp.int32)).astype(jnp.float32)
    picked = jnp.einsum("goc,ck->gko", onehot, jnp.asarray(PAIRS, dtype=jnp.float32))
    return picked.reshape(groups * 4, columns)


def size_of(axes):
    return int(np.prod([lax.axis_size(a) for a in axes]))


def shifted(x, axis, step):
    n = lax.axis_size(axis)
    return lax.ppermute(x, axis, [(i, (i + step) % n) for i in range(n)])


def swapped(x):
    return shifted(x, "core", 1)


def halves(x):
    high = lax.reduce_precision(x, 8, 7)
    return high.astype(jnp.bfloat16), (x - high).astype(jnp.bfloat16)


def line_sum(x, axis):
    total = x
    for step in range(1, lax.axis_size(axis)):
        total = total + shifted(x, axis, step)
    return total


def plane_sum(x):
    for axis in reversed(SUMMED):
        x = line_sum(x, axis)
    return x


def plane_sum_once(x):
    n = size_of(SUMMED)
    parts = lax.all_to_all(jnp.broadcast_to(x, (n, *x.shape)), SUMMED, 0, 0, tiled=True)
    return jnp.sum(parts, axis=0)


def ring_of(x, axis):
    n = lax.axis_size(axis)
    half = x.shape[0] // 2
    back, ahead = [], []
    left = right = x
    for step in range(1, n // 2):
        left = shifted(left, axis, 1)
        right = shifted(right, axis, -1)
        back.append(left)
        ahead.append(right)
    last = jnp.concatenate([shifted(left[:half], axis, 1), shifted(right[half:], axis, -1)], 0)
    return [x] + back + [last] + ahead[::-1]


def to_ring_order(x, axis):
    n = lax.axis_size(axis)
    turned = x[::-1]
    return lax.dynamic_slice_in_dim(
        jnp.concatenate([turned, turned], 0), n - 1 - lax.axis_index(axis), n, 0
    )


def other_first(x):
    mine = lax.axis_index("core")
    return jnp.where(mine == 0, x, x[::-1])


def on_device(calib, weights, codes):
    rows, features = calib.shape
    columns = weights.shape[1]
    share = size_of(SHARED)
    ring = lax.axis_size("z")
    own = columns // share

    blocks = ring_of(calib, "z")
    mask = keep_mask(codes)
    kept = mask * weights
    dropped = weights - kept

    first = lax.dot_general(
        dropped, calib, (((0,), (0,)), ((), ())),
        precision=lax.Precision.HIGHEST, preferred_element_type=jnp.float32,
    )
    sent = jnp.concatenate([first, dropped.T, mask.T], 1).reshape(share, own, -1)
    got = lax.all_to_all(sent, SHARED, 0, 0, tiled=True)
    along = plane_sum(jnp.sum(got[:, :, :features], axis=0))

    pair = got[:, :, features:].reshape(ring, 2, own, 2 * rows)
    pair = to_ring_order(pair, "z")
    pair = other_first(jnp.swapaxes(pair, 0, 1)).reshape(share, own, 2 * rows)
    drop_t = jnp.swapaxes(pair[:, :, :rows], 0, 1).reshape(own, share * rows)
    mask_t = jnp.swapaxes(pair[:, :, rows:], 0, 1).reshape(own, share * rows)

    mine = jnp.concatenate(blocks, 0)
    both = jnp.concatenate([mine, swapped(mine)], 0)
    high, low = halves(both)

    def times(vector, rest):
        up, down = halves(vector)
        stack = jnp.concatenate([up, down], 0)
        dims = (((1,), (rest,)), ((), ()))
        big = lax.dot_general(stack, high, dims, preferred_element_type=jnp.float32)
        small = lax.dot_general(stack, low, dims, preferred_element_type=jnp.float32)
        n = vector.shape[0]
        return big[:n] + (big[n:] + small[:n] + small[n:])

    def back(vector):
        return times(vector, 1) / features

    residual = mask_t * (back(along) + RIDGE * drop_t)
    direction = jnp.zeros_like(residual)
    change = jnp.zeros_like(residual)
    norm = square = None
    for step in range(ITERS):
        local = times(residual, 0)
        own_norm = jnp.sum(residual * residual, axis=1, keepdims=True)
        mixed = jnp.sum(residual * direction, axis=1, keepdims=True)
        extra = jnp.concatenate(
            [own_norm, mixed, jnp.zeros((own, LANES - 2), jnp.float32)], 1
        )
        total = plane_sum(jnp.concatenate([local, extra], 1))
        image = total[:, :features]
        new = total[:, features : features + 1]
        cross = total[:, features + 1 : features + 2]
        if step == 0:
            along, direction, square = image, residual, new
        else:
            ratio = new / norm
            along = image + ratio * along
            direction = residual + ratio * direction
            square = new + ratio * (2.0 * cross + ratio * square)
        norm = new
        alpha = norm / (jnp.sum(along * along, axis=1, keepdims=True) / features + RIDGE * square)
        change = change + alpha * direction
        if step + 1 < ITERS:
            residual = residual - alpha * (mask_t * back(along) + RIDGE * direction)

    out = jnp.swapaxes(change.reshape(own, share, rows), 0, 1)
    out = other_first(out.reshape(2, ring, own, rows))
    out = to_ring_order(jnp.swapaxes(out, 0, 1), "z")
    home = lax.all_to_all(out.reshape(share, own, rows), SHARED, 0, 0, tiled=True)
    return kept + home.reshape(columns, rows).T


def solution(mesh):
    devices = mesh.devices.reshape(8, 4, 2, mesh.shape["narrow"])
    spec = P(AXES, None)
    return jax.shard_map(
        on_device, mesh=Mesh(devices, MESH), in_specs=(spec, spec, spec), out_specs=spec,
        check_vma=False,
    )
```

```python
import jax
import jax.numpy as jnp
import numpy as np
from jax import lax
from jax.experimental import pallas as pl
from jax.experimental.pallas import tpu as pltpu
from jax.sharding import Mesh
from jax.sharding import PartitionSpec as P

ITERS = 3
RIDGE = 1.0
AXES = ("x", "z", "y", "core")
MESH = ("z", "y", "core", "x")
SHARED = ("z", "core")
SUMMED = ("y", "x")
LANES = 128
PAIRS = np.array(
    [[1, 1, 0, 0], [1, 0, 1, 0], [1, 0, 0, 1], [0, 1, 1, 0], [0, 1, 0, 1], [0, 0, 1, 1]], np.float32
)


def keep_mask(codes):
    groups, columns = codes.shape
    onehot = (codes[:, :, None] == jnp.arange(6, dtype=jnp.int32)).astype(jnp.float32)
    picked = jnp.einsum("goc,ck->gko", onehot, jnp.asarray(PAIRS, dtype=jnp.float32))
    return picked.reshape(groups * 4, columns)


def size_of(axes):
    return int(np.prod([lax.axis_size(a) for a in axes]))


def shifted(x, axis, step):
    n = lax.axis_size(axis)
    return lax.ppermute(x, axis, [(i, (i + step) % n) for i in range(n)])


def swapped(x):
    return shifted(x, "core", 1)


def exact_halves(x):
    high = x.astype(jnp.bfloat16)
    return high, (x - high.astype(jnp.float32)).astype(jnp.bfloat16)


def folded(big, small):
    n = big.shape[0] // 2
    return big[:n] + (big[n:] + small[:n] + small[n:])


def stacked(vector):
    return jnp.concatenate(exact_halves(vector), 0)


def times_tile(stack, tile, rest):
    dims = (((1,), (rest,)), ((), ()))
    return folded(
        *(lax.dot_general(stack, part, dims, preferred_element_type=jnp.float32) for part in tile)
    )


def first_kernel(count, order, *refs):
    pieces, (got, local, drop, mask, high, low) = refs[:count], refs[count:]
    rows = got.shape[2] // 2
    for block in range(got.shape[0]):
        pair = got[order[block]]
        at = slice(block * rows, block * rows + rows)
        drop[:, at] = pair[:, :rows]
        mask[:, at] = pair[:, rows:]
    start = 0
    for piece in pieces:
        at = slice(start, start + piece.shape[0])
        high[at, :], low[at, :] = exact_halves(piece[...])
        start = at.stop
    local[...] = times(drop[...], high, low, 0)


def times(vector, high, low, rest):
    return times_tile(stacked(vector), (high[...], low[...]), rest)


def sweep(high, low, along, update, out):
    features = along.shape[1]
    residual, direction = update(times(along, high, low, 1) / features)
    total = times(residual, high, low, 0)
    norm = jnp.sum(residual * residual, axis=1, keepdims=True)
    if direction is None:
        mixed = jnp.zeros_like(norm)
    else:
        mixed = jnp.sum(residual * direction, axis=1, keepdims=True)
    lane = lax.broadcasted_iota(jnp.int32, (norm.shape[0], LANES), 1)
    out[:, :features] = total
    out[:, features:] = jnp.where(lane == 0, norm, jnp.where(lane == 1, mixed, 0.0))


def start_kernel(high, low, along, drop, mask, residual, out):
    def update(back):
        new = mask[...] * (back + RIDGE * drop[...])
        residual[...] = new
        return new, None

    sweep(high, low, along[...], update, out)


def scalars_of(total, features):
    return total[:, features : features + 1], total[:, features + 1 : features + 2]


def combined(total, residual, past):
    features = total.shape[1] - LANES
    image = total[:, :features]
    new, cross = scalars_of(total, features)
    if past is None:
        along, direction, square = image, residual, new
    else:
        old_along, old_direction, norm, old_square = past
        ratio = new / norm
        along = image + ratio * old_along
        direction = residual + ratio * old_direction
        square = new + ratio * (2.0 * cross + ratio * old_square)
    alpha = new / (jnp.sum(along * along, axis=1, keepdims=True) / features + RIDGE * square)
    return along, direction, new, square, alpha


def step_kernel(high, low, total, residual, mask, *rest):
    past, outs = rest[:-6], rest[-6:]
    along_out, direction_out, change_out, scal_out, residual_out, out = outs
    old = None
    if past:
        old_along, old_direction, old_change, old_scal = (ref[...] for ref in past)
        old = (old_along, old_direction, old_scal[:, 0:1], old_scal[:, 1:2])
    before = residual[...]
    along, direction, norm, square, alpha = combined(total[...], before, old)
    along_out[...] = along
    direction_out[...] = direction
    change_out[...] = old_change + alpha * direction if past else alpha * direction
    lane = lax.broadcasted_iota(jnp.int32, scal_out.shape, 1)
    scal_out[...] = jnp.where(lane == 0, norm, square)

    def update(back):
        new = before - alpha * (mask[...] * back + RIDGE * direction)
        residual_out[...] = new
        return new, direction

    sweep(high, low, along, update, out)


IN_VMEM = pl.BlockSpec(memory_space=pltpu.VMEM)
PARAMS = pltpu.CompilerParams(vmem_limit_bytes=24 * 1024 * 1024)


def shapes_of(outs):
    return [jax.ShapeDtypeStruct(shape, jnp.float32) for shape in outs]


def cost_of(passes, rows, features, own):
    return pl.CostEstimate(
        flops=8 * passes * rows * features * own,
        bytes_accessed=4 * rows * features,
        transcendentals=0,
    )


def gathered_start(pieces, got, order):
    count = len(pieces)
    own = got.shape[1]
    rows, features = sum(piece.shape[0] for piece in pieces), pieces[0].shape[1]

    def body(order_ref, *refs):
        first_kernel(count, order_ref, *refs)

    return pl.pallas_call(
        body,
        name="first",
        out_shape=shapes_of([(own, features), (own, rows), (own, rows)])
        + [jax.ShapeDtypeStruct((rows, features), jnp.bfloat16)] * 2,
        in_specs=[pl.BlockSpec(memory_space=pltpu.SMEM)] + [IN_VMEM] * (count + 1),
        out_specs=[IN_VMEM] * 5,
        compiler_params=PARAMS,
        cost_estimate=cost_of(1, rows, features, own),
    )(order, *pieces, got)


def run(kernel, parts, vectors, outs):
    rows, features = parts[0].shape
    return pl.pallas_call(
        kernel,
        out_shape=shapes_of(outs),
        in_specs=[IN_VMEM] * (2 + len(vectors)),
        out_specs=[IN_VMEM] * len(outs),
        compiler_params=PARAMS,
        cost_estimate=cost_of(2, rows, features, outs[0][0]),
    )(*parts, *vectors)


def finish_kernel(order, total, residual, old_along, old_direction, old_change, old_scal, out):
    half, rows = out.shape[1], out.shape[2] // 2
    past = (old_along[...], old_direction[...], old_scal[:, 0:1], old_scal[:, 1:2])
    _, direction, _, _, alpha = combined(total[...], residual[...], past)
    change = old_change[...] + alpha * direction
    for block in range(out.shape[0]):
        part = change[:, block * rows : block * rows + rows]
        out[order[block]] = jnp.concatenate([part[:half], part[half:]], 1)


def finish(total, residual, along, direction, change, scal, order):
    share = order.shape[0]
    own, rows = residual.shape[0], residual.shape[1] // share
    return pl.pallas_call(
        finish_kernel,
        name="finish",
        out_shape=jax.ShapeDtypeStruct((share, own // 2, 2 * rows), jnp.float32),
        in_specs=[pl.BlockSpec(memory_space=pltpu.SMEM)] + [IN_VMEM] * 6,
        out_specs=IN_VMEM,
        compiler_params=PARAMS,
    )(order, total, residual, along, direction, change, scal)


def landed_kernel(home, kept, out):
    share, half, width = home.shape
    turned = home[...].reshape(share * half, width).T
    rows = width // 2
    out[...] = kept[...] + jnp.concatenate([turned[:rows], turned[rows:]], 1)


def landed(home, kept):
    return pl.pallas_call(
        landed_kernel,
        name="landed",
        out_shape=jax.ShapeDtypeStruct(kept.shape, jnp.float32),
        in_specs=[IN_VMEM] * 2,
        out_specs=IN_VMEM,
        compiler_params=PARAMS,
    )(home, kept)


def line_sum(x, axis):
    total = x
    for step in range(1, lax.axis_size(axis)):
        total = total + shifted(x, axis, step)
    return total


def plane_sum(x):
    for axis in reversed(SUMMED):
        x = line_sum(x, axis)
    return x


def ring_of(x, axis):
    n = lax.axis_size(axis)
    half = x.shape[0] // 2
    top, bottom = x[:half], x[half:]
    left, right = [(top, bottom)], [(top, bottom)]
    for _ in range(1, n // 2):
        (a, b), (c, d) = left[-1], right[-1]
        left.append((shifted(a, axis, 1), shifted(b, axis, 1)))
        right.append((shifted(c, axis, -1), shifted(d, axis, -1)))
    last = (shifted(left[-1][0], axis, 1), shifted(right[-1][1], axis, -1))
    blocks = [(0, (top, bottom)), (4, last)]
    for step in range(1, n // 2):
        blocks += [(step, left[step]), (n - step, right[step])]
    return blocks


def pack_kernel(*refs):
    out, start = refs[-1], 0
    for piece in refs[:-1]:
        out[start : start + piece.shape[0], :] = piece[...]
        start += piece.shape[0]


def packed(pieces):
    rows = sum(piece.shape[0] for piece in pieces)
    return pl.pallas_call(
        pack_kernel,
        name="pack",
        out_shape=jax.ShapeDtypeStruct((rows, pieces[0].shape[1]), jnp.float32),
        in_specs=[IN_VMEM] * len(pieces),
        out_specs=IN_VMEM,
        compiler_params=PARAMS,
    )(*pieces)


def on_device(calib, weights, codes):
    rows, features = calib.shape
    columns = weights.shape[1]
    share = size_of(SHARED)
    ring = lax.axis_size("z")
    own = columns // share

    mask = keep_mask(codes)
    kept = mask * weights
    dropped = weights - kept
    sent = jnp.concatenate([dropped.T, mask.T], 1).reshape(2, share, own // 2, 2 * rows)
    sent = jnp.swapaxes(sent, 0, 1).reshape(share, own, 2 * rows)
    blocks = ring_of(calib, "z")
    got = lax.all_to_all(sent, SHARED, 0, 0, tiled=True)

    core = lax.axis_index("core")
    mine = packed([part for _, pair in blocks for part in pair])
    pieces = [mine, swapped(mine)]
    far = jnp.remainder(lax.axis_index("z") - jnp.array([k for k, _ in blocks]), ring)
    order = jnp.concatenate([2 * far + core, 2 * far + 1 - core]).astype(jnp.int32)
    wide = share * rows
    vector, image, message = (own, wide), (own, features), (own, features + LANES)

    along, drop_t, mask_t, *parts = gathered_start(pieces, got, order)
    along = plane_sum(along)
    residual, local = run(start_kernel, parts, [along, drop_t, mask_t], [vector, message])
    past = []
    for _ in range(ITERS - 1):
        *past, residual, local = run(
            step_kernel, parts, [plane_sum(local), residual, mask_t, *past],
            [image, vector, vector, (own, LANES), vector, message],
        )
    spread_out = finish(plane_sum(local), residual, *past, order)
    home = lax.all_to_all(spread_out, SHARED, 0, 0, tiled=True)
    return landed(home, kept)


def solution(mesh):
    devices = mesh.devices.reshape(8, 4, 2, mesh.shape["narrow"])
    spec = P(AXES, None)
    return jax.shard_map(
        on_device, mesh=Mesh(devices, MESH), in_specs=(spec, spec, spec), out_specs=spec,
        check_vma=False,
    )
```
